32 devices in a mesh: bank: 8 (over z, core), zero: 4 (over y, x).
Axes of the slice: x: 2, y: 2, z: 4, core: 2. Of those that a mesh axis runs over, the one named last changes fastest.
Arguments:
- master_gate: float32 [64, 2048, 1408], P('bank', 'zero'), may hold values from -0.1875 to 0.1875
- master_up: float32 [64, 2048, 1408], P('bank', 'zero'), may hold values from -0.1875 to 0.1875
- master_down: float32 [64, 1408, 2048], P('bank', None, 'zero'), may hold values from -0.21875 to 0.21875
- router_weight: float32 [2048, 64], P('zero', 'bank'), may hold values from -0.125 to 0.125
- router_gain: float32 [2048], P('zero'), may hold values from 0.25 to 1.75
Outputs:
- final_gate: bfloat16 [64, 2048, 1408], P('bank', None, 'zero')
- final_up: bfloat16 [64, 2048, 1408], P('bank', None, 'zero')
- final_down: bfloat16 [64, 1408, 2048], P('bank', 'zero')
- scale_gate: float32 [64, 1408], P('bank', 'zero')
- scale_up: float32 [64, 1408], P('bank', 'zero')
- scale_down: float32 [64, 1408], P('bank', 'zero')
- serve_router: bfloat16 [2048, 64], replicated
The draws below stay inside these ranges and needn't reach their ends.
All inputs are finite; a program needn't handle non-finite values. Where the reference program divides by a largest or mean magnitude, that divisor is 1e-20 or more.
Results may differ from the reference program's by a relative error of at most 0.0013.
Values may be sent and summed in bfloat16 or wider, within the bound.
A program may use at most 192 MiB of HBM per device.

```python
import jax
import jax.numpy as jnp

EXPERTS = 64
D_MODEL = 2048
D_EXPERT = 1408


def strengthened(drawn, key, source, target, blocks, factor):
    owner, partner = [(jnp.arange(drawn.shape[axis_at]) // (drawn.shape[axis_at] // blocks)).reshape([-1 if axis == axis_at else 1 for axis in range(drawn.ndim)]) for axis_at in (source, target)]
    chosen = jax.random.permutation(key, blocks)[partner]
    strong = (owner == chosen) | (owner == (partner + blocks // 2) % blocks)
    return jnp.where(strong, factor * drawn, drawn)


def level_of(rng, extent, split, least, high):
    def one(position, parts):
        steps = jax.random.uniform(jax.random.fold_in(jax.random.fold_in(rng, 6), position), (parts,), jnp.float32, least / len(split), high / len(split))
        return jnp.repeat(jnp.exp(steps), extent[position] // parts).reshape((-1,) + (1,) * (len(extent) - position - 1))

    loudness = one(*split[0])
    for cut in split[1:]:
        loudness = loudness * one(*cut)
    return loudness


def normal_values(own_key, dims, width, reach, cuts=(), held_as=jnp.bfloat16):
    values = width * jax.random.normal(own_key, dims, jnp.float32)
    if cuts:
        values = values * level_of(own_key, dims, cuts, -0.22, 0.18)
    return jnp.clip(values, -reach, reach).astype(held_as)


def noise_with(own_key, extent, scale, reach, pieces, heavy, dtype=jnp.bfloat16):
    entries = scale * jax.random.normal(own_key, extent, jnp.float32)
    if pieces:
        entries = entries * level_of(own_key, extent, pieces, -0.22, 0.18)
    return jnp.clip(strengthened(entries, jax.random.fold_in(own_key, 3), *heavy), -reach, reach).astype(dtype)


def setup_inputs(seed: int = 0) -> dict:
    keys = jax.random.split(jax.random.key(seed), 6)
    return {
        "master_gate": noise_with(keys[0], (EXPERTS, D_MODEL, D_EXPERT), D_MODEL ** -0.5, 0.1875, ((0, 8), (1, 4)), (1, 2, 4, 2.0), jnp.float32),
        "master_up": noise_with(keys[1], (EXPERTS, D_MODEL, D_EXPERT), D_MODEL ** -0.5, 0.1875, ((0, 8), (1, 4)), (1, 2, 4, 2.0), jnp.float32),
        "master_down": noise_with(keys[2], (EXPERTS, D_EXPERT, D_MODEL), D_EXPERT ** -0.5, 0.21875, ((0, 8), (2, 4)), (2, 1, 4, 2.0), jnp.float32),
        "router_weight": normal_values(keys[3], (D_MODEL, EXPERTS), D_MODEL ** -0.5, 0.125, ((0, 4), (1, 8)), jnp.float32),
        "router_gain": jnp.clip(1.0 + 0.15 * jax.random.normal(keys[4], (D_MODEL,), jnp.float32), 0.25, 1.75),
    }


def reference(master_gate, master_up, master_down, router_weight, router_gain):
    scale_gate = jnp.sum(jnp.abs(master_gate), axis=1) / D_MODEL
    final_gate = (master_gate / jnp.expand_dims(scale_gate, 1)).astype(jnp.bfloat16)
    scale_up = jnp.sum(jnp.abs(master_up), axis=1) / D_MODEL
    final_up = (master_up / jnp.expand_dims(scale_up, 1)).astype(jnp.bfloat16)
    scale_down = jnp.sum(jnp.abs(master_down), axis=2) / D_MODEL
    final_down = (master_down / jnp.expand_dims(scale_down, 2)).astype(jnp.bfloat16)
    serve_router = (router_weight * router_gain[:, None]).astype(jnp.bfloat16)
    return final_gate, final_up, final_down, scale_gate, scale_up, scale_down, serve_router
```

```python
import jax
import jax.numpy as jnp
from jax import lax
from jax.sharding import PartitionSpec as P


def exchange(wide, scale, parts):
    experts, rows, width = wide.shape
    narrow = (wide / scale[:, :, None]).astype(jnp.bfloat16)
    cut = narrow.reshape(experts, parts, rows // parts, width).transpose(1, 0, 2, 3)
    return lax.all_to_all(cut, "zero", split_axis=0, concat_axis=0, tiled=True), cut


def merged(blocks):
    return jnp.concatenate([blocks[p] for p in range(blocks.shape[0])], axis=2)


def local(parts, master_gate, master_up, master_down, router_weight, router_gain):
    experts, rows, inner = master_gate.shape
    d_model = rows * parts
    sums = jnp.stack(
        [
            jnp.sum(jnp.abs(master_gate), axis=1),
            jnp.sum(jnp.abs(master_up), axis=1),
            jnp.sum(jnp.abs(master_down), axis=2),
        ]
    )
    part_router = (router_weight * router_gain[:, None]).astype(jnp.bfloat16).T
    router = lax.all_gather(part_router, ("bank", "zero"), axis=0, tiled=False)
    sums, router = lax.optimization_barrier((sums, router))
    every = lax.all_gather(sums, "zero", axis=0, tiled=False)
    scales = jnp.sum(every, axis=0) / d_model
    router = router.reshape(-1, parts, experts, rows).transpose(0, 2, 1, 3)
    serve_router = router.reshape(-1, d_model).T

    got_down, cut = exchange(master_down, scales[2], parts)
    master_gate, cut = lax.optimization_barrier((master_gate, cut))
    got_gate, cut = exchange(master_gate.transpose(0, 2, 1), scales[0], parts)
    master_up, cut = lax.optimization_barrier((master_up, cut))
    got_up, cut = exchange(master_up.transpose(0, 2, 1), scales[1], parts)

    final_down = merged(got_down)
    final_gate = merged(got_gate).transpose(0, 2, 1)
    final_up = merged(got_up).transpose(0, 2, 1)
    own = lax.dynamic_slice_in_dim(
        scales, lax.axis_index("zero") * (inner // parts), inner // parts, axis=2
    )
    return (final_gate, final_up, final_down, own[0], own[1], own[2], serve_router)


def solution(mesh):
    placed = (
        P("bank", "zero", None),
        P("bank", "zero", None),
        P("bank", None, "zero"),
        P("zero", "bank"),
        P("zero"),
    )
    parts = mesh.shape["zero"]
    return jax.shard_map(
        lambda *arrays: local(parts, *arrays),
        mesh=mesh,
        in_specs=placed,
        out_specs=(
            P("bank", None, "zero"),
            P("bank", None, "zero"),
            P("bank", "zero", None),
            P("bank", "zero"),
            P("bank", "zero"),
            P("bank", "zero"),
            P(),
        ),
        check_vma=False,
    )
```
